32 devices in a mesh: row: 4 (over z), col: 4 (over y, core), rep: 2 (over x).
Axes of the slice: x: 2, y: 2, z: 4, core: 2. Of those that a mesh axis runs over, the one named last changes fastest.
Arguments:
- amplitudes: bfloat16 [1024, 8192], P('row', 'col'), may hold values from -6 to 6
- intermediate: bfloat16 [8192, 1024], P('row', 'col'), may hold values from -0.0625 to 0.0625
Outputs:
- residual: float32 [8, 4, 32, 1024], P(None, 'col', None, ('row', 'rep'))
The draws below stay inside these ranges and needn't reach their ends.
All inputs are finite; a program needn't handle non-finite values.
Results may differ from the reference program's by a relative error of at most 0.0029.
Values may be sent and summed in bfloat16 or wider, within the bound.
A program may use at most 128 MiB of HBM per device.

```python
import jax
import jax.numpy as jnp

KC_WIDTH = 8192
PAIR_DEV = 32
PAIRS = 1024
N_ROW = 4
N_COL = 4
N_REP = 2


def block_levels(rng, shape, cuts, least, largest):
    def one(dim, blocks):
        heights = jax.random.uniform(jax.random.fold_in(jax.random.fold_in(rng, 6), dim), (blocks,), jnp.float32, least / len(cuts), largest / len(cuts))
        return jnp.repeat(jnp.exp(heights), shape[dim] // blocks).reshape((-1,) + (1,) * (len(shape) - dim - 1))

    loudness = one(*cuts[0])
    for cut in cuts[1:]:
        loudness = loudness * one(*cut)
    return loudness


def scatter_about(stream_key, dims, width, bound, split=(), held_as=jnp.bfloat16):
    values = jax.random.normal(stream_key, dims, jnp.float32) * width
    if len(split) > 0:
        values = block_levels(stream_key, dims, split, -0.22, 0.18) * values
    return jnp.clip(values, min=-bound, max=bound).astype(held_as)


def setup_inputs(seed: int = 0) -> dict:
    keys = jax.random.split(jax.random.key(seed), 3)
    return {
        "amplitudes": scatter_about(keys[0], (PAIRS, KC_WIDTH), 1.0, 6.0, ((0, 4), (1, 4))),
        "intermediate": scatter_about(keys[1], (KC_WIDTH, PAIRS), KC_WIDTH ** -0.5, 0.0625, ((0, 4), (1, 4))),
    }


def reference(amplitudes, intermediate):
    cycle = jnp.dot(amplitudes, intermediate, preferred_element_type=jnp.float32).astype(jnp.bfloat16)
    widened = cycle.astype(jnp.float32)
    symmetric = widened + widened.T
    return symmetric.reshape(N_ROW * N_REP, N_COL, PAIR_DEV, PAIRS)
```

```python
import functools

import jax
import jax.numpy as jnp
from jax import lax
from jax.experimental import pallas as pl
from jax.experimental.pallas import tpu as pltpu
from jax.sharding import PartitionSpec as P

MESH = pl.DeviceIdType.MESH


def general(amplitudes, intermediate):
    rows_axis = lax.axis_size("row")
    cols_axis = lax.axis_size("col")
    depth_axis = lax.axis_size("rep")
    layer_index = lax.axis_index("rep")
    owner_rows = rows_axis * depth_axis
    fold_count = owner_rows // cols_axis
    local_rows = amplitudes.shape[0]
    band_rows = local_rows // depth_axis
    local_cols = intermediate.shape[1]
    slice_width = local_cols // owner_rows
    own_rows = lax.dynamic_slice_in_dim(amplitudes, layer_index * band_rows, band_rows, 0)
    all_weights = lax.all_gather(intermediate, "row", axis=0, tiled=True)
    summed = jnp.dot(
        lax.all_gather(own_rows, "col", axis=1, tiled=True),
        all_weights,
        preferred_element_type=jnp.float32,
    )
    cycle = summed.astype(jnp.bfloat16)
    spread_block = cycle.reshape(band_rows, fold_count, cols_axis, slice_width)
    direct = lax.all_to_all(spread_block, "col", split_axis=2, concat_axis=1, tiled=True).reshape(
        band_rows, owner_rows, slice_width
    )
    stacked = cycle.reshape(cols_axis, slice_width, fold_count, cols_axis * slice_width)
    mirror = lax.all_to_all(
        lax.all_to_all(stacked, "col", split_axis=0, concat_axis=2, tiled=True),
        ("row", "rep"),
        split_axis=2,
        concat_axis=0,
        tiled=True,
    )
    mirror_part = mirror.reshape(owner_rows, slice_width, band_rows).astype(jnp.float32)
    direct_part = jnp.transpose(direct, (1, 2, 0)).astype(jnp.float32)
    return (mirror_part + direct_part).reshape(owner_rows, 1, slice_width, band_rows)


def kernel(
    sizes, a_hbm, w_hbm, o_ref,
    a_v, w_v, relay, abuf, part, rbuf, cyc, turn, mrecv, drecv,
    in_sem, s_all, q_rly, q_z, q_y, q_c, q_r, q_m, q_d, near_sem, far_sem, side_sem,
):
    rows, cols, depth, n = sizes
    r, c, x = lax.axis_index("row"), lax.axis_index("col"), lax.axis_index("rep")
    y, u = c // 2, c % 2
    oy, ou, ox = 1 - y, 1 - u, 1 - x
    band, kc = a_v.shape
    line = band // 2
    ch = line // n
    half = kc // 2
    strip = o_ref.shape[2]
    lanes = o_ref.shape[3]
    f32 = jnp.float32

    def khalf(v):
        return pl.ds(v * half, half)

    def mine(v):
        return pl.ds(pl.multiple_of(v * half, half), half)

    def line_rows(side):
        return pl.ds(pl.multiple_of(side * line, line), line)

    def hbm_rows(side):
        return pl.ds(pl.multiple_of(x * band + side * line, line), line)

    loads = (
        pltpu.make_async_copy(a_hbm.at[hbm_rows(oy)], a_v.at[line_rows(oy)], in_sem.at[0]),
        pltpu.make_async_copy(a_hbm.at[hbm_rows(y)], a_v.at[line_rows(y)], in_sem.at[1]),
        pltpu.make_async_copy(w_hbm, w_v, in_sem.at[2]),
    )
    for load in loads:
        load.start()

    barrier = pltpu.get_barrier_semaphore()
    core_mate, y_mate, x_mate = (r, y * 2 + ou, x), (r, oy * 2 + u, x), (r, c, ox)
    has_low, has_high = r > 0, r < rows - 1

    def signal(sem, to):
        pl.semaphore_signal(sem, inc=1, device_id=to, device_id_type=MESH)

    for to in (y_mate, core_mate, (r, oy * 2 + ou, x), x_mate):
        signal(barrier, to)

    @pl.when(has_low)
    def _():
        for v in range(2):
            signal(barrier, (r - 1, y * 2 + v, x))

    @pl.when(has_high)
    def _():
        for v in range(2):
            signal(barrier, (r + 1, y * 2 + v, x))

    inner = jnp.logical_and(has_low, has_high)
    pl.semaphore_wait(barrier, jnp.where(inner, 8, 6))

    pending = []
    count = [0]

    def send(source, target, rsem, to, same=None, local=None, only=None):
        index = count[0]
        count[0] += 1
        copy = pltpu.make_async_remote_copy(
            src_ref=source, dst_ref=target, send_sem=s_all.at[index], recv_sem=rsem,
            device_id=to, device_id_type=MESH,
        )
        if same is None:
            copy.start()
            pending.append((copy, None))
            return

        @pl.when(same)
        def _():
            pltpu.make_async_copy(source if local is None else local, target, rsem).start()

        @pl.when(jnp.logical_not(same))
        def _():
            copy.start()

        pending.append((copy, jnp.logical_not(same)))

    def arrived(target, recv):
        pltpu.make_async_copy(target, target, recv).wait()

    loads[0].wait()
    for i in range(n):
        at = pl.ds(pl.multiple_of(oy * line + i * ch, ch), ch)
        send(a_v.at[at], relay.at[i], q_rly.at[i], y_mate)

    signal(side_sem, x_mate)

    @pl.when(inner)
    def _():
        signal(near_sem, (r - 1, c, x))
        signal(near_sem, (r + 1, c, x))

    pl.semaphore_wait(near_sem, 1)

    @pl.when(r == 1)
    def _():
        signal(far_sem, (r - 1, c, x))

    @pl.when(r == rows - 2)
    def _():
        signal(far_sem, (r + 1, c, x))

    pl.when(jnp.logical_not(inner))(lambda: pl.semaphore_wait(far_sem, 1))

    loads[1].wait()

    def piece(i):
        return y * n + i

    for i in range(n):
        at = pl.ds(pl.multiple_of(y * line + i * ch, ch), ch)
        for v in range(2):
            send(
                a_v.at[at, khalf(v)], abuf.at[piece(i), r, :, khalf(v)], q_z.at[i, r],
                (c, y * 2 + v, x), jnp.logical_and(c == r, u == v),
            )

    far = oy * 2 + u
    order = (r, r + 1 - 2 * (r % 2), (r + rows // 2) % rows, rows - 1 - r)

    def relay_on(i):
        arrived(relay.at[i], q_rly.at[i])
        for v in range(2):
            send(
                relay.at[i, :, khalf(v)], abuf.at[piece(i), r, :, khalf(v)], q_z.at[i, r],
                (far, y * 2 + v, x), jnp.logical_and(far == r, u == v),
            )

    def to_core(j):
        ref = abuf.at[j, :, :, mine(u)]
        send(ref, ref, q_c.at[j], core_mate)

    def from_z(i):
        j = piece(i)
        for s in order:
            ref = abuf.at[j, s, :, mine(u)]
            arrived(ref, q_z.at[i, s])
            send(ref, ref, q_y.at[i, s], y_mate)
        to_core(j)

    def from_y(i):
        j = oy * n + i
        for s in order:
            arrived(abuf.at[j, s, :, mine(u)], q_y.at[i, s])
        to_core(j)

    def product(j):
        arrived(abuf.at[j, :, :, mine(ou)], q_c.at[j])
        value = jnp.dot(
            abuf[j].reshape(rows * ch, kc), w_v[...], preferred_element_type=f32
        )
        part[j] = value.reshape(rows, ch, value.shape[1])
        for s in order[1:]:
            send(part.at[j, s], rbuf.at[j, r], q_r.at[j, r], (s, c, x))

    def total(j):
        value = part[j, r]
        for s in order[1:]:
            arrived(rbuf.at[j, s], q_r.at[j, s])
            value = value + rbuf[j, s]
        cyc[pl.ds(pl.multiple_of(j * ch, ch), ch), :] = value.astype(jnp.bfloat16)

    per = strip // ch

    def finish(side, g):
        m = side * (cols // 2) + g
        for i in range(per):
            total(side * n + g * per + i)
        for px in range(depth):
            send(
                cyc.at[pl.ds(pl.multiple_of(m * strip, strip), strip), pl.ds(px * lanes, lanes)],
                mrecv.at[r * depth + x], q_m.at[r * depth + x], (c, m, px),
                jnp.logical_and(jnp.logical_and(c == r, m == c), px == x),
            )

    relay_on(0)
    relay_on(1)
    relay_on(2)
    from_z(0)
    relay_on(3)
    loads[2].wait()
    pl.semaphore_wait(side_sem, 1)
    from_z(1)
    product(y * n)
    from_y(0)
    from_z(2)
    product(y * n + 1)
    product(oy * n)
    from_y(1)
    from_z(3)
    product(y * n + 2)
    product(oy * n + 1)
    from_y(2)
    product(y * n + 3)
    product(oy * n + 2)
    from_y(3)
    product(oy * n + 3)
    finish(y, 0)
    finish(oy, 0)
    finish(y, 1)
    finish(oy, 1)

    turn[...] = jnp.transpose(cyc[...].astype(f32)).astype(jnp.bfloat16)
    for to in range(cols):
        for b in range(2):
            at = c * 2 + b
            send(
                turn.at[pl.ds(b * lanes + to * strip, strip)], drecv.at[at], q_d.at[at], (r, to, x), c == to,
            )

    for i in range(rows * depth):
        arrived(mrecv.at[i], q_m.at[i])
        arrived(drecv.at[i], q_d.at[i])
        o_ref[i, 0] = mrecv[i].astype(f32) + drecv[i].astype(f32)

    for copy, sent in pending:
        if sent is None:
            copy.wait_send()
        else:
            pl.when(sent)(copy.wait_send)


def planned(sizes, amplitudes, intermediate):
    rows, cols, depth, n = sizes
    kc, width = intermediate.shape
    band = amplitudes.shape[0] // depth
    owners = rows * depth
    strip = width // owners
    ch = band // (2 * n)
    bf16, f32 = jnp.bfloat16, jnp.float32
    dma, plain = pltpu.SemaphoreType.DMA, pltpu.SemaphoreType.REGULAR
    return pl.pallas_call(
        functools.partial(kernel, sizes),
        out_shape=jax.ShapeDtypeStruct((owners, 1, strip, band), f32),
        in_specs=[pl.BlockSpec(memory_space=pl.ANY)] * 2,
        out_specs=pl.BlockSpec(memory_space=pltpu.VMEM),
        scratch_shapes=[
            pltpu.VMEM((band, kc), bf16),
            pltpu.VMEM((kc, width), bf16),
            pltpu.VMEM((n, ch, kc), bf16),
            pltpu.VMEM((2 * n, rows, ch, kc), bf16),
            pltpu.VMEM((2 * n, rows, ch, width), f32),
            pltpu.VMEM((2 * n, rows, ch, width), f32),
            pltpu.VMEM((band, width), bf16),
            pltpu.VMEM((width, band), bf16),
            pltpu.VMEM((owners, strip, band), bf16),
            pltpu.VMEM((owners, strip, band), bf16),
            dma((3,)), dma((128,)), dma((n,)), dma((n, rows)), dma((n, rows)), dma((2 * n,)),
            dma((2 * n, rows)), dma((owners,)), dma((owners,)), plain, plain, plain,
        ],
        compiler_params=pltpu.CompilerParams(collective_id=0, has_side_effects=True),
    )(amplitudes, intermediate)


def solution(mesh):
    rows, cols, depth = (mesh.shape[name] for name in ("row", "col", "rep"))

    def local(amplitudes, intermediate):
        square = rows == cols == 2 * depth and depth == 2
        band, width = amplitudes.shape[0] // depth, intermediate.shape[1]
        fits = amplitudes.shape[0] == width and band % 128 == 0 and amplitudes.shape[1] == intermediate.shape[0]
        if square and fits and band == 128:
            return planned((rows, cols, depth, 4), amplitudes, intermediate)
        return general(amplitudes, intermediate)

    in_specs = (P("row", "col"), P("row", "col"))
    out_specs = P(None, "col", None, ("row", "rep"))
    return jax.shard_map(local, mesh=mesh, in_specs=in_specs, out_specs=out_specs, check_vma=False)
```

```python
import functools

import jax
import jax.numpy as jnp
from jax import lax
from jax.experimental import pallas as pl
from jax.experimental.pallas import tpu as pltpu
from jax.sharding import PartitionSpec as P

MESH = pl.DeviceIdType.MESH


def general(amplitudes, intermediate):
    rows_axis = lax.axis_size("row")
    cols_axis = lax.axis_size("col")
    depth_axis = lax.axis_size("rep")
    layer_index = lax.axis_index("rep")
    owner_rows = rows_axis * depth_axis
    fold_count = owner_rows // cols_axis
    local_rows = amplitudes.shape[0]
    band_rows = local_rows // depth_axis
    local_cols = intermediate.shape[1]
    slice_width = local_cols // owner_rows
    own_rows = lax.dynamic_slice_in_dim(amplitudes, layer_index * band_rows, band_rows, 0)
    all_weights = lax.all_gather(intermediate, "row", axis=0, tiled=True)
    summed = jnp.dot(
        lax.all_gather(own_rows, "col", axis=1, tiled=True),
        all_weights,
        preferred_element_type=jnp.float32,
    )
    cycle = summed.astype(jnp.bfloat16)
    spread_block = cycle.reshape(band_rows, fold_count, cols_axis, slice_width)
    direct = lax.all_to_all(spread_block, "col", split_axis=2, concat_axis=1, tiled=True).reshape(
        band_rows, owner_rows, slice_width
    )
    stacked = cycle.reshape(cols_axis, slice_width, fold_count, cols_axis * slice_width)
    mirror = lax.all_to_all(
        lax.all_to_all(stacked, "col", split_axis=0, concat_axis=2, tiled=True),
        ("row", "rep"),
        split_axis=2,
        concat_axis=0,
        tiled=True,
    )
    mirror_part = mirror.reshape(owner_rows, slice_width, band_rows).astype(jnp.float32)
    direct_part = jnp.transpose(direct, (1, 2, 0)).astype(jnp.float32)
    return (mirror_part + direct_part).reshape(owner_rows, 1, slice_width, band_rows)


RELAY, OWN, RELAYED, KEPT, ACROSS, NEAR, AWAY, PARTIAL, OUTWARD, PASSED, MIRROR, DIRECT, LAST = range(13)


def kernel(
    sizes, a_hbm, w_hbm, o_ref,
    a_v, w_v, relay, abuf, part, acc, rbuf, cyc, turn, mrecv, drecv,
    in_sem, s_all, q_rly, q_z, q_y, q_near, q_away, q_acc, q_r0, q_r1, q_r2, q_out, near_sem, far_sem, side_sem,
):
    rows, cols, depth, n = sizes
    r, c, x = lax.axis_index("row"), lax.axis_index("col"), lax.axis_index("rep")
    y, u = c // 2, c % 2
    oy, ou, ox = 1 - y, 1 - u, 1 - x
    band, kc = a_v.shape
    line = band // 2
    ch = line // n
    half = kc // 2
    strip = o_ref.shape[2]
    lanes = o_ref.shape[3]
    per = n // 2
    f32 = jnp.float32

    def khalf(v):
        return pl.ds(v * half, half)

    def mine(v):
        return pl.ds(pl.multiple_of(v * half, half), half)

    def line_rows(side):
        return pl.ds(pl.multiple_of(side * line, line), line)

    def chunk_rows(side, i):
        return pl.ds(pl.multiple_of(side * line + i * ch, ch), ch)

    def hbm_rows(side):
        return pl.ds(pl.multiple_of(x * band + side * line, line), line)

    loads = (
        pltpu.make_async_copy(a_hbm.at[hbm_rows(oy)], a_v.at[line_rows(oy)], in_sem.at[0]),
        pltpu.make_async_copy(a_hbm.at[hbm_rows(y)], a_v.at[line_rows(y)], in_sem.at[1]),
        pltpu.make_async_copy(w_hbm, w_v, in_sem.at[2]),
    )
    for load in loads:
        load.start()

    barrier = pltpu.get_barrier_semaphore()
    core_mate, y_mate, x_mate = (r, y * 2 + ou, x), (r, oy * 2 + u, x), (r, c, ox)
    has_low, has_high = r > 0, r < rows - 1

    def signal(sem, to):
        pl.semaphore_signal(sem, inc=1, device_id=to, device_id_type=MESH)

    for to in (y_mate, core_mate, (r, oy * 2 + ou, x), x_mate):
        signal(barrier, to)

    @pl.when(has_low)
    def _():
        for v in range(2):
            signal(barrier, (r - 1, y * 2 + v, x))

    @pl.when(has_high)
    def _():
        for v in range(2):
            signal(barrier, (r + 1, y * 2 + v, x))

    inner = jnp.logical_and(has_low, has_high)
    outer = jnp.logical_not(inner)
    pl.semaphore_wait(barrier, jnp.where(inner, 8, 6))

    mate, near, away = r + 1 - 2 * (r % 2), 2 * (r // 2), 2 - 2 * (r // 2)
    home = y == r // 2
    over = oy * 2 + u

    def remote(source, target, group, rsem, to):
        return pltpu.make_async_remote_copy(
            src_ref=source, dst_ref=target, send_sem=s_all.at[group], recv_sem=rsem,
            device_id=to, device_id_type=MESH,
        )

    def send(source, target, group, rsem, to, same=None):
        copy = remote(source, target, group, rsem, to)
        if same is None:
            copy.start()
        else:
            pl.when(same)(lambda: pltpu.make_async_copy(source, target, rsem).start())
            pl.when(jnp.logical_not(same))(copy.start)

    def arrived(target, recv):
        pltpu.make_async_copy(target, target, recv).wait()

    loads[0].wait()
    for i in range(n):
        send(a_v.at[chunk_rows(oy, i)], relay.at[i], RELAY, q_rly.at[i], y_mate)

    signal(side_sem, x_mate)

    @pl.when(inner)
    def _():
        signal(near_sem, (r - 1, c, x))
        signal(near_sem, (r + 1, c, x))

    reach = jnp.abs(c - r)
    pl.when(reach > 1)(lambda: pl.semaphore_wait(near_sem, 1))
    pl.when(reach > 2)(lambda: pl.semaphore_wait(far_sem, 1))
    loads[1].wait()

    def slot(i, plane):
        return jnp.where(plane == r, i // per, jnp.where(plane == mate, 2 + i // per, 4 + i))

    def along(source, i, plane, group):
        for v in range(2):
            send(
                source(khalf(v)), abuf.at[y * n + i, r, :, khalf(v)], group, q_z.at[slot(i, plane)],
                (plane, y * 2 + v, x), jnp.logical_and(plane == r, u == v),
            )

    def own(i):
        along(lambda ks: a_v.at[chunk_rows(y, i), ks], i, c, OWN)

    own(0)
    own(1)
    pl.when(reach <= 1)(lambda: pl.semaphore_wait(near_sem, 1))
    pl.when(r == 1)(lambda: signal(far_sem, (r - 1, c, x)))
    pl.when(r == rows - 2)(lambda: signal(far_sem, (r + 1, c, x)))
    pl.when(jnp.logical_and(outer, reach <= 2))(lambda: pl.semaphore_wait(far_sem, 1))

    def relay_on(i):
        arrived(relay.at[i], q_rly.at[i])
        along(lambda ks: relay.at[i, :, ks], i, over, RELAYED)

    def keep(i):
        for v in range(2):
            source, target = a_v.at[chunk_rows(oy, i), khalf(v)], abuf.at[oy * n + i, r, :, khalf(v)]
            recv = q_y.at[i // per]
            copy = remote(source, target, KEPT, recv, core_mate)
            here = jnp.logical_and(c == r, u == v)
            pl.when(here)(lambda: pltpu.make_async_copy(source, target, recv).start())
            pl.when(jnp.logical_and(c == r, u != v))(copy.start)

    def own_block(side, g):
        return abuf.at[pl.ds(side * n + g * per, per), r, :, mine(u)]

    def mate_block(side, g):
        return abuf.at[pl.ds(side * n + g * per, per), mate, :, mine(u)]

    def away_block(j, v):
        return abuf.at[j, pl.ds(away, 2), :, mine(v)]

    def own_z(g):
        ref = own_block(y, g)
        arrived(ref, q_z.at[g])
        copy = remote(ref, ref, ACROSS, q_y.at[g], y_mate)
        pl.when(home)(copy.start)

    def mate_z(g):
        ref = mate_block(y, g)
        arrived(ref, q_z.at[2 + g])
        send(ref, ref, ACROSS, q_y.at[2 + g], y_mate)

    def near_to_core(side, g):
        ref = abuf.at[pl.ds(side * n + g * per, per), pl.ds(near, 2), :, mine(u)]
        send(ref, ref, NEAR, q_near.at[side * 2 + g], core_mate)

    def away_to_core(j):
        send(away_block(j, u), away_block(j, u), AWAY, q_away.at[j], core_mate)

    def away_z(i):
        ref = away_block(y * n + i, u)
        arrived(ref, q_z.at[4 + i])
        send(ref, ref, ACROSS, q_y.at[4 + i], y_mate)
        away_to_core(y * n + i)

    def near_y(g):
        arrived(own_block(oy, g), q_y.at[g])
        arrived(mate_block(oy, g), q_y.at[2 + g])
        near_to_core(oy, g)

    def away_y(i):
        arrived(away_block(oy * n + i, u), q_y.at[4 + i])
        away_to_core(oy * n + i)

    def near_product(side, g):
        chunks, pair = pl.ds(side * n + g * per, per), pl.ds(near, 2)
        arrived(abuf.at[chunks, pair, :, mine(ou)], q_near.at[side * 2 + g])
        value = jnp.dot(
            abuf[chunks, pair].reshape(2 * per * ch, kc), w_v[...], preferred_element_type=f32
        )
        part[chunks, pair] = value.reshape(per, 2, ch, value.shape[1])
        send(part.at[chunks, mate], rbuf.at[chunks, 0], PARTIAL, q_r0.at[side * 2 + g], (mate, c, x))

    def product(side, i):
        j = side * n + i
        pair = pl.ds(away, 2)
        arrived(away_block(j, ou), q_away.at[j])
        value = jnp.dot(
            abuf[j, pair].reshape(2 * ch, kc), w_v[...], preferred_element_type=f32
        )
        part[j, pair] = value.reshape(2, ch, value.shape[1])
        if i < n - 1:
            outward = remote(part.at[j, pair], acc.at[side * (n - 1) + i], OUTWARD, q_acc.at[side * (n - 1) + i], (mate, c, x))
            pl.when(outer)(outward.start)
            return
        for f in range(2):
            send(part.at[j, away + f], rbuf.at[j, 1 + r % 2], LAST, q_r2.at[side], (away + f, c, x))

    def pass_on(side, i):
        j, m = side * n + i, side * 2 + i // per
        copies = [
            remote(part.at[j, away + f], rbuf.at[j, 1], PASSED, q_r1.at[m], (away + f, c, x)) for f in range(2)
        ]

        @pl.when(inner)
        def _():
            arrived(acc.at[side * (n - 1) + i], q_acc.at[side * (n - 1) + i])
            for f in range(2):
                part[j, away + f] = part[j, away + f] + acc[side * (n - 1) + i, f]
                copies[f].start()

    def finish(side, g):
        m = side * 2 + g
        chunks = pl.ds(side * n + g * per, per)
        arrived(rbuf.at[chunks, 0], q_r0.at[m])
        through = per - g
        arrived(rbuf.at[pl.ds(side * n + g * per, through), 1], q_r1.at[m])
        early = pl.ds(side * n + g * per, through)
        value = part[early, r] + rbuf[early, 0] + rbuf[early, 1]
        if g:
            j = side * n + n - 1
            arrived(rbuf.at[j, pl.ds(1, 2)], q_r2.at[side])
            ends = part[j, r] + rbuf[j, 0] + rbuf[j, 1] + rbuf[j, 2]
            value = jnp.concatenate([value, ends[None]], axis=0)
        at = pl.ds(pl.multiple_of(m * strip, strip), strip)
        cyc[at, :] = value.reshape(strip, value.shape[2]).astype(jnp.bfloat16)
        for px in range(depth):
            send(
                cyc.at[at, pl.ds(px * lanes, lanes)], mrecv.at[r * depth + x], MIRROR, q_out.at[0], (c, m, px),
                jnp.logical_and(jnp.logical_and(c == r, m == c), px == x),
            )

    def flush(group, ref):
        pltpu.make_async_copy(ref, ref, s_all.at[group]).wait()

    relay_on(0)
    own(2)
    relay_on(1)
    own(3)
    for i in range(n):
        keep(i)
    own_z(0)
    relay_on(2)
    relay_on(3)
    own_z(1)
    mate_z(0)
    near_to_core(y, 0)
    away_z(0)
    mate_z(1)
    near_to_core(y, 1)
    loads[2].wait()
    near_product(y, 0)
    product(y, 0)
    away_z(1)
    away_y(0)
    near_product(y, 1)
    near_y(0)
    product(y, 1)
    away_z(2)
    pl.semaphore_wait(side_sem, 1)
    product(oy, 0)
    pass_on(y, 0)
    away_y(1)
    near_product(oy, 0)
    pass_on(y, 1)
    away_z(3)
    product(y, 2)
    near_y(1)
    product(oy, 1)
    pass_on(oy, 0)
    away_y(2)
    near_product(oy, 1)
    product(y, 3)
    pass_on(y, 2)
    pass_on(oy, 1)
    away_y(3)
    product(oy, 2)
    finish(y, 0)
    product(oy, 3)
    pass_on(oy, 2)
    finish(oy, 0)
    finish(y, 1)
    finish(oy, 1)

    turn[...] = jnp.transpose(cyc[...].astype(f32)).astype(jnp.bfloat16)
    for to in range(cols):
        for b in range(2):
            at = c * 2 + b
            send(
                turn.at[pl.ds(b * lanes + to * strip, strip)], drecv.at[at], DIRECT, q_out.at[1], (r, to, x), c == to,
            )

    flush(RELAY, relay)
    for group, plane in ((OWN, c), (RELAYED, over)):
        pl.when(plane == r)(lambda: flush(group, relay.at[:, :, khalf(0)]))
        pl.when(plane != r)(lambda: flush(group, relay))
    pl.when(c == r)(lambda: flush(KEPT, relay.at[:, :, khalf(0)]))
    pl.when(home)(lambda: flush(ACROSS, abuf.at[pl.ds(0, n), :, :, khalf(0)]))
    pl.when(jnp.logical_not(home))(lambda: flush(ACROSS, abuf.at[pl.ds(0, n), pl.ds(0, rows - 1), :, khalf(0)]))
    flush(NEAR, abuf.at[:, pl.ds(0, 2), :, khalf(0)])
    flush(AWAY, abuf.at[:, pl.ds(0, 2), :, khalf(0)])
    flush(PARTIAL, part.at[:, 0])
    pl.when(outer)(lambda: flush(OUTWARD, acc))
    pl.when(inner)(lambda: flush(PASSED, acc))
    flush(LAST, rbuf.at[pl.ds(0, 2), pl.ds(1, 2)])

    arrived(mrecv, q_out.at[0])
    arrived(drecv, q_out.at[1])
    for i in range(rows * depth):
        o_ref[i, 0] = mrecv[i].astype(f32) + drecv[i].astype(f32)

    pl.when(c == r)(lambda: flush(MIRROR, mrecv.at[pl.ds(0, rows * depth - 1)]))
    pl.when(c != r)(lambda: flush(MIRROR, mrecv))
    flush(DIRECT, drecv.at[pl.ds(0, rows * depth - 2)])


def planned(sizes, amplitudes, intermediate):
    rows, cols, depth, n = sizes
    kc, width = intermediate.shape
    band = amplitudes.shape[0] // depth
    owners = rows * depth
    strip = width // owners
    ch = band // (2 * n)
    bf16, f32 = jnp.bfloat16, jnp.float32
    dma, plain = pltpu.SemaphoreType.DMA, pltpu.SemaphoreType.REGULAR
    return pl.pallas_call(
        functools.partial(kernel, sizes),
        out_shape=jax.ShapeDtypeStruct((owners, 1, strip, band), f32),
        in_specs=[pl.BlockSpec(memory_space=pl.ANY)] * 2,
        out_specs=pl.BlockSpec(memory_space=pltpu.VMEM),
        scratch_shapes=[
            pltpu.VMEM((band, kc), bf16),
            pltpu.VMEM((kc, width), bf16),
            pltpu.VMEM((n, ch, kc), bf16),
            pltpu.VMEM((2 * n, rows, ch, kc), bf16),
            pltpu.VMEM((2 * n, rows, ch, width), f32),
            pltpu.VMEM((2 * (n - 1), 2, ch, width), f32),
            pltpu.VMEM((2 * n, 3, ch, width), f32),
            pltpu.VMEM((band, width), bf16),
            pltpu.VMEM((width, band), bf16),
            pltpu.VMEM((owners, strip, band), bf16),
            pltpu.VMEM((owners, strip, band), bf16),
            dma((3,)), dma((13,)), dma((n,)), dma((4 + n,)), dma((4 + n,)), dma((4,)), dma((2 * n,)), dma((2 * n,)),
            dma((4,)), dma((4,)), dma((2,)), dma((2,)), plain, plain, plain,
        ],
        compiler_params=pltpu.CompilerParams(
            collective_id=0, has_side_effects=True, vmem_limit_bytes=56_000_000
        ),
    )(amplitudes, intermediate)


def solution(mesh):
    rows, cols, depth = (mesh.shape[name] for name in ("row", "col", "rep"))

    def local(amplitudes, intermediate):
        square = rows == cols == 2 * depth and depth == 2
        band, width = amplitudes.shape[0] // depth, intermediate.shape[1]
        fits = amplitudes.shape[0] == width and band % 128 == 0 and amplitudes.shape[1] == intermediate.shape[0]
        if square and fits and band == 128:
            return planned((rows, cols, depth, 4), amplitudes, intermediate)
        return general(amplitudes, intermediate)

    in_specs = (P("row", "col"), P("row", "col"))
    out_specs = P(None, "col", None, ("row", "rep"))
    return jax.shard_map(local, mesh=mesh, in_specs=in_specs, out_specs=out_specs, check_vma=False)
```
